32 devices in a mesh: seq: 16 (over z, y, x), tp: 2 (over core).
Axes of the slice: x: 2, y: 2, z: 4, core: 2. Of those that a mesh axis runs over, the one named last changes fastest.
Arguments:
- query_rows: bfloat16 [2048, 2048], P('seq', 'tp'), may hold values from -350 to 350
- key_rows: bfloat16 [2048, 512], P('seq', 'tp'), may hold values from -6 to 6
- stored_value_rows: bfloat16 [2048, 512], P('seq', 'tp'), may hold values from -6 to 6
- output_grad: bfloat16 [2048, 2048], P('seq', 'tp'), may hold values from -96 to 96
- layer_input: bfloat16 [2048, 4096], P('seq', 'tp'), may hold values from -6 to 6
- key_matrix: bfloat16 [4096, 512], P(None, 'tp'), may hold values from -0.09375 to 0.09375
- value_matrix: bfloat16 [4096, 512], P(None, 'tp'), may hold values from -0.09375 to 0.09375
- run_placement: int32 [16, 16], replicated, may hold values from 0 to 15, as said below
Outputs:
- query_grad: bfloat16 [2048, 2048], P('seq', 'tp')
- input_grad: bfloat16 [2048, 4096], P('seq', 'tp')
- key_weight_grad: float32 [4096, 512], P('seq', 'tp')
- value_weight_grad: float32 [4096, 512], P('seq', 'tp')
The draws below stay inside these ranges and needn't reach their ends.
Inputs may be any that keep to these rules, and one draw needn't show every extreme that they name: `run_placement`: row j gives, for each storing index d of seq, the slot within sequence block j of the 8 consecutive positions that d holds; every row is a permutation of 0 to 15.
All inputs are finite; a program needn't handle non-finite values.
Results may differ from the reference program's by a relative error of at most 0.0081.
Values may be sent and summed in bfloat16 or wider, within the bound.
A program may use at most 128 MiB of HBM per device.

```python
import math
import jax
import jax.numpy as jnp
from jax import lax

MODEL_WIDTH = 4096
HEAD_SIZE = 128
WINDOW_LENGTH = 4096
QUERY_HEADS = 16
KEY_VALUE_HEADS = 4
TOK_DEV = 128
SEQUENCE_TOKENS = 2048
N_SEQ = 16


def slot_table(key):
    row_keys = jax.random.split(jax.random.fold_in(key, 101), N_SEQ)
    return jax.vmap(lambda row_key: jax.random.permutation(row_key, N_SEQ))(row_keys).astype(jnp.int32)


def key_sample(key):
    start_offset = jnp.clip(jax.random.normal(jax.random.fold_in(key, 202), (SEQUENCE_TOKENS, KEY_VALUE_HEADS, HEAD_SIZE), jnp.float32), -4.0, 4.0)
    return start_offset


def draw_run_placement(key, part):
    return slot_table(key)


def draw_key_rows(key, part):
    return key_sample(key).reshape(SEQUENCE_TOKENS, KEY_VALUE_HEADS * HEAD_SIZE).astype(jnp.bfloat16)


def draw_query_rows(key, part):
    start_offset = jnp.clip(jax.random.normal(jax.random.fold_in(key, 303), (SEQUENCE_TOKENS, QUERY_HEADS * HEAD_SIZE), jnp.float32), -4.0, 4.0)
    return start_offset.astype(jnp.bfloat16)


def spiked(drawn, key, source, target, parts, factor):
    owner, partner = [(jnp.arange(drawn.shape[dim]) // (drawn.shape[dim] // parts)).reshape([-1 if axis == dim else 1 for axis in range(drawn.ndim)]) for dim in (source, target)]
    chosen = jax.random.permutation(key, parts)[partner]
    strong = (owner == chosen) | (owner == (partner + parts // 2) % parts)
    return jnp.where(strong, factor * drawn, drawn)


def level_of(own_key, dims, shards, low, largest):
    def one(dim, blocks):
        steps = jax.random.uniform(jax.random.fold_in(jax.random.fold_in(own_key, 6), dim), (blocks,), jnp.float32, low / len(shards), largest / len(shards))
        return jnp.repeat(jnp.exp(steps), dims[dim] // blocks).reshape((-1,) + (1,) * (len(dims) - dim - 1))

    level = one(*shards[0])
    for cut in shards[1:]:
        level = level * one(*cut)
    return level


def normal_values(key, dims, width, reach, cuts=(), kind=jnp.bfloat16):
    drawn = width * jax.random.normal(key, dims, jnp.float32)
    if cuts:
        drawn = drawn * level_of(key, dims, cuts, -0.22, 0.18)
    return jnp.clip(drawn, -reach, reach).astype(kind)


def gaussian_with(rng, extent, scale, bound, cuts, heavy, held_as=jnp.bfloat16):
    array = scale * jax.random.normal(rng, extent, jnp.float32)
    if cuts:
        array = array * level_of(rng, extent, cuts, -0.22, 0.18)
    return jnp.clip(spiked(array, jax.random.fold_in(rng, 3), *heavy), -bound, bound).astype(held_as)


def setup_inputs(seed: int = 0) -> dict:
    key_list = jax.random.split(jax.random.key(seed), 9)
    return {
        "query_rows": draw_query_rows(jax.random.fold_in(key_list[8], 71), 0),
        "key_rows": draw_key_rows(jax.random.fold_in(key_list[8], 71), 0),
        "stored_value_rows": normal_values(key_list[2], (SEQUENCE_TOKENS, KEY_VALUE_HEADS * HEAD_SIZE), 1.0, 6.0, ((0, 16), (1, 2))),
        "output_grad": normal_values(key_list[3], (SEQUENCE_TOKENS, QUERY_HEADS * HEAD_SIZE), 16.0, 96.0, ((0, 16), (1, 2))),
        "layer_input": gaussian_with(key_list[4], (SEQUENCE_TOKENS, MODEL_WIDTH), 1.0, 6.0, ((0, 16), (1, 2)), (0, 1, 16, 2.0)),
        "key_matrix": normal_values(key_list[5], (MODEL_WIDTH, KEY_VALUE_HEADS * HEAD_SIZE), MODEL_WIDTH ** -0.5, 0.09375, ((1, 2),)),
        "value_matrix": normal_values(key_list[6], (MODEL_WIDTH, KEY_VALUE_HEADS * HEAD_SIZE), MODEL_WIDTH ** -0.5, 0.09375, ((1, 2),)),
        "run_placement": draw_run_placement(jax.random.fold_in(key_list[8], 71), 0),
    }


masked_value = -1e+30

def to_sequence(matrix, run_placement):
    run_rows = TOK_DEV // N_SEQ
    columns = matrix.shape[1]
    stored = matrix.reshape(N_SEQ, N_SEQ, run_rows, columns).transpose(1, 0, 2, 3)
    inverse = jnp.argsort(run_placement, axis=1).astype(jnp.int32)
    picked = jnp.take_along_axis(stored, inverse[:, :, None, None], axis=1)
    return picked.reshape(SEQUENCE_TOKENS, columns)

def into_stored_order(matrix, run_placement):
    run_rows = TOK_DEV // N_SEQ
    columns = matrix.shape[1]
    blocks = matrix.reshape(N_SEQ, N_SEQ, run_rows, columns)
    picked = jnp.take_along_axis(blocks, run_placement.astype(jnp.int32)[:, :, None, None], axis=1)
    return picked.transpose(1, 0, 2, 3).reshape(SEQUENCE_TOKENS, columns)

def rounded(values):
    return lax.optimization_barrier(values.astype(jnp.bfloat16)).astype(jnp.float32)

def reference(query_rows, key_rows, stored_value_rows, output_grad, layer_input, key_matrix, value_matrix, run_placement):
    score_scale = 1.0 / math.sqrt(HEAD_SIZE)
    query_group = QUERY_HEADS // KEY_VALUE_HEADS
    queries = to_sequence(query_rows, run_placement)
    grads = to_sequence(output_grad, run_placement)
    empty_rows = jnp.zeros((WINDOW_LENGTH, KEY_VALUE_HEADS * HEAD_SIZE), jnp.bfloat16)
    padded_keys = jnp.concatenate([empty_rows, to_sequence(key_rows, run_placement)], axis=0)
    padded_values = jnp.concatenate([empty_rows, to_sequence(stored_value_rows, run_placement)], axis=0)
    window_keys = WINDOW_LENGTH + TOK_DEV

    def one_block(carry, block_index):
        leading_row = block_index * TOK_DEV
        q_block = lax.dynamic_slice_in_dim(queries, leading_row, TOK_DEV, 0).astype(jnp.float32).reshape(TOK_DEV, QUERY_HEADS, HEAD_SIZE)
        g_block = lax.dynamic_slice_in_dim(grads, leading_row, TOK_DEV, 0).astype(jnp.float32).reshape(TOK_DEV, QUERY_HEADS, HEAD_SIZE)
        key_block = lax.dynamic_slice_in_dim(padded_keys, leading_row, window_keys, 0).astype(jnp.float32).reshape(window_keys, KEY_VALUE_HEADS, HEAD_SIZE)
        value_block = lax.dynamic_slice_in_dim(padded_values, leading_row, window_keys, 0).astype(jnp.float32).reshape(window_keys, KEY_VALUE_HEADS, HEAD_SIZE)
        k_heads = jnp.repeat(key_block, query_group, axis=1)
        v_heads = jnp.repeat(value_block, query_group, axis=1)
        query_pos = leading_row + jnp.arange(TOK_DEV, dtype=jnp.int32)
        key_pos = leading_row - WINDOW_LENGTH + jnp.arange(window_keys, dtype=jnp.int32)
        in_window = (key_pos[None, :] <= query_pos[:, None]) & (key_pos[None, :] > query_pos[:, None] - WINDOW_LENGTH) & (key_pos[None, :] >= 0)
        logits = jnp.einsum('qhd,khd->hqk', q_block, k_heads) * score_scale
        row_top = lax.optimization_barrier(jnp.max(jnp.where(in_window[None], logits, masked_value), axis=2))
        exponent = jnp.where(in_window[None], jnp.exp(logits - row_top[:, :, None]), 0.0)
        row_total = lax.optimization_barrier(jnp.sum(exponent, axis=2))
        log_total = row_top + jnp.log(row_total)
        prob_grad = jnp.einsum('qhd,khd->hqk', g_block, v_heads)
        row_delta = lax.optimization_barrier(jnp.sum(exponent * prob_grad, axis=2)) / row_total
        probs = jnp.where(in_window[None], jnp.exp(logits - log_total[:, :, None]), 0.0)
        score_grad = probs * (prob_grad - row_delta[:, :, None])
        probs_b = rounded(probs)
        score_b = rounded(score_grad)
        query_part = (jnp.einsum('hqk,khd->qhd', score_b, k_heads) * score_scale).astype(jnp.bfloat16)
        key_portion = jnp.einsum('hqk,qhd->khd', score_b, q_block) * score_scale
        key_portion = key_portion.reshape(window_keys, KEY_VALUE_HEADS, query_group, HEAD_SIZE).sum(axis=2).reshape(window_keys, KEY_VALUE_HEADS * HEAD_SIZE)
        value_portion = jnp.einsum('hqk,qhd->khd', probs_b, g_block)
        value_portion = value_portion.reshape(window_keys, KEY_VALUE_HEADS, query_group, HEAD_SIZE).sum(axis=2).reshape(window_keys, KEY_VALUE_HEADS * HEAD_SIZE)
        update = jnp.concatenate([key_portion, value_portion], axis=1)
        current = lax.dynamic_slice_in_dim(carry, leading_row, window_keys, 0)
        carry = lax.dynamic_update_slice_in_dim(carry, current + update, leading_row, 0)
        return (carry, query_part.reshape(TOK_DEV, QUERY_HEADS * HEAD_SIZE))
    gradient_start = jnp.zeros((WINDOW_LENGTH + SEQUENCE_TOKENS, 2 * KEY_VALUE_HEADS * HEAD_SIZE), jnp.float32)
    final, query_parts = lax.scan(one_block, gradient_start, jnp.arange(N_SEQ, dtype=jnp.int32))
    key_value_pair = final[WINDOW_LENGTH:]
    key_gradient = into_stored_order(key_value_pair[:, :KEY_VALUE_HEADS * HEAD_SIZE].astype(jnp.bfloat16), run_placement)
    value_gradient = into_stored_order(key_value_pair[:, KEY_VALUE_HEADS * HEAD_SIZE:].astype(jnp.bfloat16), run_placement)
    query_grad = into_stored_order(query_parts.reshape(SEQUENCE_TOKENS, QUERY_HEADS * HEAD_SIZE), run_placement)
    key_weight_grad = jnp.dot(layer_input.T, key_gradient, preferred_element_type=jnp.float32)
    value_weight_grad = jnp.dot(layer_input.T, value_gradient, preferred_element_type=jnp.float32)
    input_grad = jnp.dot(key_gradient, key_matrix.T, preferred_element_type=jnp.float32)
    input_grad = (input_grad + jnp.dot(value_gradient, value_matrix.T, preferred_element_type=jnp.float32)).astype(jnp.bfloat16)
    return (query_grad, input_grad, key_weight_grad, value_weight_grad)
```

```python
import functools
import math

import jax
import jax.numpy as jnp
from jax import lax
from jax.experimental import pallas as pl
from jax.experimental.pallas import tpu as pltpu
from jax.sharding import PartitionSpec as P

HEAD_SIZE = 128
WINDOW_LENGTH = 4096
GROUP = 4
CHUNK = 256
MASKED = -1e30
NT = (((1,), (1,)), ((), ()))
NN = (((1,), (0,)), ((), ()))
TN = (((0,), (0,)), ((), ()))


def dot(a, b, dims):
    return lax.dot_general(a, b, dims, preferred_element_type=jnp.float32)


def attention_kernel(kv_local, q_ref, g_ref, kv_ref, qpos_ref, kpos_ref, dq_ref, dkv_ref, s_ref):
    rows = q_ref.shape[0]
    keys = kv_ref.shape[0]
    kv_width = kv_local * HEAD_SIZE
    wide = GROUP * rows
    chunks = keys // CHUNK
    scale = 1.0 / math.sqrt(HEAD_SIZE)
    qpos = jnp.concatenate([qpos_ref[...]] * GROUP, axis=1)
    for c in range(kv_local):
        first = c * GROUP
        heads = [slice((first + i) * HEAD_SIZE, (first + i + 1) * HEAD_SIZE) for i in range(GROUP)]
        q4 = jnp.concatenate([q_ref[:, h] for h in heads], axis=0)
        g4 = jnp.concatenate([g_ref[:, h] for h in heads], axis=0)
        k_cols = slice(c * HEAD_SIZE, (c + 1) * HEAD_SIZE)
        v_cols = slice(kv_width + c * HEAD_SIZE, kv_width + (c + 1) * HEAD_SIZE)

        def forward(i, carry):
            top, total, weighted = carry
            at = pl.ds(pl.multiple_of(i * CHUNK, CHUNK), CHUNK)
            kpos = kpos_ref[at, :]
            seen = (kpos <= qpos) & (kpos > qpos - WINDOW_LENGTH)
            s = jnp.where(seen, dot(kv_ref[at, k_cols], q4, NT) * scale, MASKED)
            dp = dot(kv_ref[at, v_cols], g4, NT)
            s_ref[at, :] = s
            new_top = jnp.maximum(top, jnp.max(s, axis=0, keepdims=True))
            e = jnp.exp(s - new_top)
            factor = jnp.exp(top - new_top)
            total = total * factor + jnp.sum(e, axis=0, keepdims=True)
            weighted = weighted * factor + jnp.sum(e * dp, axis=0, keepdims=True)
            return new_top, total, weighted

        zero = jnp.zeros((1, wide), jnp.float32)
        top, total, weighted = lax.fori_loop(
            0, chunks, forward, (jnp.full((1, wide), MASKED, jnp.float32), zero, zero)
        )
        lse = top + jnp.log(total)
        delta = weighted / total

        def backward(i, acc):
            at = pl.ds(pl.multiple_of(i * CHUNK, CHUNK), CHUNK)
            prob = jnp.exp(s_ref[at, :] - lse)
            dp = dot(kv_ref[at, v_cols], g4, NT)
            ds = (prob * (dp - delta)).astype(jnp.bfloat16)
            dkv_ref[at, k_cols] = (dot(ds, q4, NN) * scale).astype(dkv_ref.dtype)
            dkv_ref[at, v_cols] = dot(prob.astype(jnp.bfloat16), g4, NN).astype(dkv_ref.dtype)
            return acc + dot(kv_ref[at, k_cols], ds, TN)

        acc = lax.fori_loop(0, chunks, backward, jnp.zeros((HEAD_SIZE, wide), jnp.float32))
        dq = (jnp.transpose(acc) * scale).astype(jnp.bfloat16)
        for i, h in enumerate(heads):
            dq_ref[:, h] = dq[i * rows : (i + 1) * rows]


def attention(q, g, kv, qpos, kpos, grad_type):
    rows, width = q.shape
    keys, kv_cols = kv.shape
    wide = GROUP * rows
    vmem = pl.BlockSpec(memory_space=pltpu.VMEM)
    return pl.pallas_call(
        functools.partial(attention_kernel, kv_cols // (2 * HEAD_SIZE)),
        out_shape=(
            jax.ShapeDtypeStruct((rows, width), jnp.bfloat16),
            jax.ShapeDtypeStruct((keys, kv_cols), grad_type),
        ),
        in_specs=[vmem] * 5,
        out_specs=(vmem, vmem),
        scratch_shapes=[pltpu.VMEM((keys, wide), jnp.float32)],
        compiler_params=pltpu.CompilerParams(vmem_limit_bytes=60 * 2**20),
    )(q, g, kv, qpos, kpos)


def positions(run_placement, rows_here):
    seq_count = run_placement.shape[0]
    run_rows = rows_here // seq_count
    block = jnp.arange(seq_count, dtype=jnp.int32)[:, None] * rows_here
    start = jnp.transpose(block + run_placement * run_rows)
    return start[:, :, None] + jnp.arange(run_rows, dtype=jnp.int32)


def local(
    query_rows,
    key_rows,
    stored_value_rows,
    output_grad,
    layer_input,
    key_matrix,
    value_matrix,
    run_placement,
):
    seq_index = lax.axis_index("seq")
    rows_here = query_rows.shape[0]
    kv_width = key_rows.shape[1]
    pos = positions(run_placement, rows_here)
    kpos = pos.reshape(-1, 1)
    qpos = lax.dynamic_index_in_dim(pos, seq_index, 0, keepdims=False).reshape(1, rows_here)
    own_kv = jnp.concatenate([key_rows, stored_value_rows], axis=1)
    kv_all = lax.all_gather(own_kv, "seq", axis=0, tiled=True)
    full_input = lax.all_gather(layer_input, "tp", axis=1, tiled=True)
    input_columns = lax.all_to_all(full_input, "seq", split_axis=1, concat_axis=0, tiled=True)
    query_grad, partial_kv = attention(query_rows, output_grad, kv_all, qpos, kpos, jnp.float32)
    kv_grad = lax.psum_scatter(partial_kv, "seq", scatter_dimension=0, tiled=True).astype(jnp.bfloat16)
    partial_input = dot(kv_grad[:, :kv_width], key_matrix, NT) + dot(
        kv_grad[:, kv_width:], value_matrix, NT
    )
    input_grad = lax.psum_scatter(partial_input, "tp", scatter_dimension=1, tiled=True).astype(
        jnp.bfloat16
    )
    weight_rows = dot(input_columns, lax.all_gather(kv_grad, "seq", axis=0, tiled=True), TN)
    return (query_grad, input_grad, weight_rows[:, :kv_width], weight_rows[:, kv_width:])


def solution(mesh):
    placed = (P("seq", "tp"),) * 5 + (P(None, "tp"), P(None, "tp"), P())
    return jax.shard_map(
        local,
        mesh=mesh,
        in_specs=placed,
        out_specs=(P("seq", "tp"),) * 4,
        check_vma=False,
    )
```

```python
import math

import jax
import jax.numpy as jnp
from jax import lax
from jax.experimental import pallas as pl
from jax.experimental.pallas import tpu as pltpu
from jax.sharding import PartitionSpec as P

HEAD_SIZE = 128
WINDOW_LENGTH = 4096
GROUP = 4
CHUNK = 256
MASKED = -1e30
NT = (((1,), (1,)), ((), ()))
NN = (((1,), (0,)), ((), ()))
TN = (((0,), (0,)), ((), ()))
MESH = pl.DeviceIdType.MESH


def dot(a, b, dims):
    return lax.dot_general(a, b, dims, preferred_element_type=jnp.float32)


def flip(index, bit):
    return index + bit - 2 * bit * ((index // bit) % 2)


def bit_orders(count):
    bits = []
    while count > 1:
        count //= 2
        bits.append(count)
    return (bits[:-2] + bits[-2:][::-1], bits)


def step_kernel(
    q_ref, g_ref, k_ref, v_ref, qpos_ref, kpos_ref, x_ref, km_ref, vm_ref,
    dq_ref, all_ref, pair_ref, cols_ref, km_out, vm_out,
    kv_ref, part_ref, land_ref, s_ref,
    send_sem, recv_sem, x_send, x_recv, side_send, side_recv, local_sem,
):
    n = lax.axis_size("seq")
    me = lax.axis_index("seq")
    tp = lax.axis_index("tp")
    rows = q_ref.shape[0]
    keys = kv_ref.shape[0]
    kv_width = k_ref.shape[1]
    kv_local = kv_width // HEAD_SIZE
    features = x_ref.shape[1]
    half = n // 2
    x_width = cols_ref.shape[1]
    block_width = features // half
    orders = bit_orders(n)
    stages = len(orders[0])
    scale = 1.0 / math.sqrt(HEAD_SIZE)
    other = {"seq": me, "tp": 1 - tp}
    groups = []
    for c in range(kv_local):
        groups.append((slice(c * HEAD_SIZE, (c + 1) * HEAD_SIZE), orders[0]))
        groups.append((slice(kv_width + c * HEAD_SIZE, kv_width + (c + 1) * HEAD_SIZE), orders[1]))

    barrier = pltpu.get_barrier_semaphore()
    for step in range(1, n):
        pl.semaphore_signal(
            barrier, inc=1, device_id={"seq": (me + step) % n, "tp": tp}, device_id_type=MESH
        )
    pl.semaphore_signal(barrier, inc=1, device_id=other, device_id_type=MESH)
    pl.semaphore_wait(barrier, n)

    def block_of(order, ident):
        index = me
        for stage, bit in enumerate(order):
            if (ident >> stage) & 1:
                index = flip(index, bit)
        return index

    def span(index):
        return pl.ds(pl.multiple_of(index * rows, rows), rows)

    sent = []

    def send(phase, g, stage, ident, src, dst):
        copy = pltpu.make_async_remote_copy(
            src_ref=src,
            dst_ref=dst,
            send_sem=send_sem.at[phase, g, 2**stage + ident],
            recv_sem=recv_sem.at[phase, g, 2**stage + ident],
            device_id={"seq": flip(me, groups[g][1][stage]), "tp": tp},
            device_id_type=MESH,
        )
        copy.start()
        sent.append(copy)
        return copy

    def gather(phase, buffer, own):
        flying = {}

        def forward(g, ident, first):
            cols, order = groups[g]
            place = buffer.at[span(block_of(order, ident)), cols]
            src = own(g) if ident == 0 else place
            for stage in range(first, stages):
                flying[g, stage, ident] = send(phase, g, stage, ident, src, place)

        for g in range(len(groups)):
            forward(g, 0, 0)
        for stage in range(stages):
            for ident in range(2**stage):
                for g in range(len(groups)):
                    flying[g, stage, ident].wait_recv()
                    forward(g, 2**stage + ident, stage + 1)

    def own_input(g):
        cols = groups[g][0]
        if cols.start < kv_width:
            return k_ref.at[:, cols]
        return v_ref.at[:, slice(cols.start - kv_width, cols.stop - kv_width)]

    kv_ref[span(me), :kv_width] = k_ref[...]
    kv_ref[span(me), kv_width:] = v_ref[...]
    gather(0, kv_ref, own_input)

    side = []
    for i, (src, dst) in enumerate(((km_ref, km_out), (vm_ref, vm_out))):
        copy = pltpu.make_async_remote_copy(
            src_ref=src.at[pl.ds(pl.multiple_of((1 - tp) * features, features), features), :],
            dst_ref=dst,
            send_sem=side_send.at[i],
            recv_sem=side_recv.at[i],
            device_id=other,
            device_id_type=MESH,
        )
        copy.start()
        side.append(copy)

    def columns_of(target):
        start = ((target % half) * block_width) // x_width * x_width
        return x_ref.at[:, pl.ds(pl.multiple_of(start, x_width), x_width)]

    def x_copy(target, slot, source):
        return pltpu.make_async_remote_copy(
            src_ref=columns_of(target),
            dst_ref=cols_ref.at[span(me), :],
            send_sem=x_send.at[slot],
            recv_sem=x_recv.at[source],
            device_id={"seq": target, "tp": tp},
            device_id_type=MESH,
        )

    holder = tp == me // half
    own_columns = pltpu.make_async_copy(columns_of(me), cols_ref.at[span(me), :], local_sem)

    @pl.when(holder)
    def _():
        own_columns.start()

    for slot in range(half):
        target = tp * half + (me + slot) % half

        @pl.when(target != me)
        def _():
            x_copy(target, slot, me).start()

    qpos = jnp.concatenate([qpos_ref[...]] * GROUP, axis=1)
    wide = GROUP * rows
    chunks = keys // CHUNK
    moving = {}

    def reduce_send(g, stage, ident):
        cols, order = groups[g]
        moving[g, stage, ident] = send(
            1,
            g,
            stage,
            ident,
            part_ref.at[span(block_of(order, 2**stage + ident)), cols],
            land_ref.at[slice((2**stage + ident) * rows, (2**stage + ident + 1) * rows), cols],
        )

    for c in range(kv_local):
        first = c * GROUP
        heads = [slice((first + i) * HEAD_SIZE, (first + i + 1) * HEAD_SIZE) for i in range(GROUP)]
        q4 = jnp.concatenate([q_ref[:, h] for h in heads], axis=0)
        g4 = jnp.concatenate([g_ref[:, h] for h in heads], axis=0)
        k_cols = slice(c * HEAD_SIZE, (c + 1) * HEAD_SIZE)
        v_cols = slice(kv_width + c * HEAD_SIZE, kv_width + (c + 1) * HEAD_SIZE)

        def forward(i, carry):
            top, total, weighted = carry
            at = pl.ds(pl.multiple_of(i * CHUNK, CHUNK), CHUNK)
            kpos = kpos_ref[at, :]
            seen = (kpos <= qpos) & (kpos > qpos - WINDOW_LENGTH)
            s = jnp.where(seen, dot(kv_ref[at, k_cols], q4, NT) * scale, MASKED)
            dp = dot(kv_ref[at, v_cols], g4, NT)
            s_ref[at, :] = s
            new_top = jnp.maximum(top, jnp.max(s, axis=0, keepdims=True))
            e = jnp.exp(s - new_top)
            factor = jnp.exp(top - new_top)
            total = total * factor + jnp.sum(e, axis=0, keepdims=True)
            weighted = weighted * factor + jnp.sum(e * dp, axis=0, keepdims=True)
            return new_top, total, weighted

        zero = jnp.zeros((1, wide), jnp.float32)
        top, total, weighted = lax.fori_loop(
            0, chunks, forward, (jnp.full((1, wide), MASKED, jnp.float32), zero, zero)
        )
        lse = top + jnp.log(total)
        delta = weighted / total

        def backward(i, acc):
            at = pl.ds(pl.multiple_of(i * CHUNK, CHUNK), CHUNK)
            prob = jnp.exp(s_ref[at, :] - lse)
            dp = dot(kv_ref[at, v_cols], g4, NT)
            ds = (prob * (dp - delta)).astype(jnp.bfloat16)
            part_ref[at, k_cols] = (dot(ds, q4, NN) * scale).astype(jnp.bfloat16)
            part_ref[at, v_cols] = dot(prob.astype(jnp.bfloat16), g4, NN).astype(jnp.bfloat16)
            return acc + dot(kv_ref[at, k_cols], ds, TN)

        acc = lax.fori_loop(0, chunks, backward, jnp.zeros((HEAD_SIZE, wide), jnp.float32))
        dq = (jnp.transpose(acc) * scale).astype(jnp.bfloat16)
        for i, h in enumerate(heads):
            dq_ref[:, h] = dq[i * rows : (i + 1) * rows]
        for ident in range(2 ** (stages - 1)):
            for g in (2 * c, 2 * c + 1):
                reduce_send(g, stages - 1, ident)

    @pl.when(holder)
    def _():
        own_columns.wait()
        for step in range(1, n):
            x_copy(me, 0, (me + step) % n).wait_recv()

    relay = pltpu.make_async_remote_copy(
        src_ref=cols_ref,
        dst_ref=cols_ref,
        send_sem=side_send.at[2],
        recv_sem=side_recv.at[2],
        device_id=other,
        device_id_type=MESH,
    )

    @pl.when(holder)
    def _():
        relay.start()

    def add(g, stage, ident, out_ref):
        cols, order = groups[g]
        moving[g, stage, ident].wait_recv()
        at = span(block_of(order, ident))
        slot = 2**stage + ident
        landed = land_ref[slot * rows : (slot + 1) * rows, cols].astype(jnp.float32)
        out_ref[at, cols] = (part_ref[at, cols].astype(jnp.float32) + landed).astype(jnp.bfloat16)

    for stage in range(stages - 1, 0, -1):
        middle = 2 ** (stage - 1)
        for g in range(len(groups)):
            for ident in range(middle, 2 * middle):
                add(g, stage, ident, part_ref)
            for ident in range(middle):
                reduce_send(g, stage - 1, ident)
        for g in range(len(groups)):
            for ident in range(middle):
                add(g, stage, ident, part_ref)
    for g in range(len(groups)):
        add(g, 0, 0, all_ref)
    mate = pltpu.make_async_remote_copy(
        src_ref=all_ref.at[span(me), :],
        dst_ref=pair_ref,
        send_sem=side_send.at[3],
        recv_sem=side_recv.at[3],
        device_id=other,
        device_id_type=MESH,
    )
    mate.start()
    gather(2, all_ref, lambda g: all_ref.at[span(me), groups[g][0]])

    for copy in sent:
        copy.wait_send()
    for copy in side + [mate]:
        copy.wait()
    for slot in range(half):
        target = tp * half + (me + slot) % half

        @pl.when(target != me)
        def _():
            x_copy(target, slot, me).wait_send()

    @pl.when(holder)
    def _():
        relay.wait_send()

    @pl.when(tp != me // half)
    def _():
        relay.wait_recv()


def step(n, q, g, k, v, qpos, kpos, x, km, vm):
    rows, width = q.shape
    kv_width = k.shape[1]
    features = x.shape[1]
    keys = n * rows
    x_width = max(2 * features // n, 128)
    groups = 2 * kv_width // HEAD_SIZE
    vmem = pl.BlockSpec(memory_space=pltpu.VMEM)
    hbm = pl.BlockSpec(memory_space=pl.ANY)
    kind = jnp.bfloat16
    dma = pltpu.SemaphoreType.DMA
    return pl.pallas_call(
        step_kernel,
        out_shape=(
            jax.ShapeDtypeStruct((rows, width), kind),
            jax.ShapeDtypeStruct((keys, 2 * kv_width), kind),
            jax.ShapeDtypeStruct((rows, 2 * kv_width), kind),
            jax.ShapeDtypeStruct((keys, x_width), kind),
            jax.ShapeDtypeStruct((features, kv_width), kind),
            jax.ShapeDtypeStruct((features, kv_width), kind),
        ),
        in_specs=[vmem] * 6 + [hbm] * 3,
        out_specs=(vmem, vmem, vmem, hbm, hbm, hbm),
        scratch_shapes=[
            pltpu.VMEM((keys, 2 * kv_width), kind),
            pltpu.VMEM((keys, 2 * kv_width), kind),
            pltpu.VMEM((keys, 2 * kv_width), kind),
            pltpu.VMEM((keys, GROUP * rows), jnp.float32),
            dma((3, groups, n)),
            dma((3, groups, n)),
            dma((n // 2,)),
            dma((n,)),
            dma((4,)),
            dma((4,)),
            dma,
        ],
        compiler_params=pltpu.CompilerParams(
            vmem_limit_bytes=63 * 2**20, collective_id=0, has_side_effects=True
        ),
    )(q, g, k, v, qpos, kpos, x, km, vm)


def positions(run_placement, rows_here):
    seq_count = run_placement.shape[0]
    run_rows = rows_here // seq_count
    block = jnp.arange(seq_count, dtype=jnp.int32)[:, None] * rows_here
    start = jnp.transpose(block + run_placement * run_rows)
    return start[:, :, None] + jnp.arange(run_rows, dtype=jnp.int32)


def local(
    query_rows,
    key_rows,
    stored_value_rows,
    output_grad,
    layer_input,
    key_matrix,
    value_matrix,
    run_placement,
):
    seq_index = lax.axis_index("seq")
    rows_here = query_rows.shape[0]
    kv_width = key_rows.shape[1]
    pos = positions(run_placement, rows_here)
    kpos = pos.reshape(-1, 1)
    qpos = lax.dynamic_index_in_dim(pos, seq_index, 0, keepdims=False).reshape(1, rows_here)
    seq_count = run_placement.shape[0]
    query_grad, kv_all, kv_mate, columns, key_far, value_far = step(
        seq_count,
        query_rows,
        output_grad,
        key_rows,
        stored_value_rows,
        qpos,
        kpos,
        layer_input,
        key_matrix,
        value_matrix,
    )
    features = layer_input.shape[1]
    tp_index = lax.axis_index("tp")
    kv_grad = lax.dynamic_slice_in_dim(kv_all, seq_index * rows_here, rows_here, 0)
    key_near = lax.dynamic_slice_in_dim(key_matrix, tp_index * features, features, 0)
    value_near = lax.dynamic_slice_in_dim(value_matrix, tp_index * features, features, 0)
    input_grad = (
        dot(kv_grad[:, :kv_width], key_near, NT)
        + dot(kv_grad[:, kv_width:], value_near, NT)
        + dot(kv_mate[:, :kv_width], key_far, NT)
        + dot(kv_mate[:, kv_width:], value_far, NT)
    ).astype(jnp.bfloat16)
    block_width = 2 * features // seq_count
    shift = (seq_index * block_width) % columns.shape[1]
    columns = lax.dynamic_slice_in_dim(columns, shift, block_width, 1)
    key_weight = dot(columns, kv_all[:, :kv_width], TN)
    value_weight = dot(columns, kv_all[:, kv_width:], TN)
    return (query_grad, input_grad, key_weight, value_weight)


def solution(mesh):
    placed = (P("seq", "tp"),) * 5 + (P(None, "tp"), P(None, "tp"), P())
    return jax.shard_map(
        local,
        mesh=mesh,
        in_specs=placed,
        out_specs=(P("seq", "tp"),) * 4,
        check_vma=False,
    )
```
